16 devices in a mesh: rep: 2 (over y, z), dp: 8 (over x, core).
Axes of the slice: x: 4, y: 2, z: 1, core: 2. Of those that a mesh axis runs over, the one named last changes fastest.
The devices are a block of a 4x4x8 slice.
Arguments:
- patches: bfloat16 [512, 256, 588], P(('rep', 'dp')), parts along dimension 0
- w_patch: bfloat16 [588, 384], P(None, 'dp')
- b_patch: bfloat16 [384], P('dp')
- pos_emb: bfloat16 [256, 384], P('dp')
- ln_scale: bfloat16 [384], P('dp')
- w_q: bfloat16 [384, 384], P('dp')
- w_k: bfloat16 [384, 384], P('dp')
- w_v: bfloat16 [384, 384], P('dp')
- q_scale: bfloat16 [64], replicated
- k_scale: bfloat16 [64], replicated
- w_out: bfloat16 [384, 384], P('dp')
- b_out: bfloat16 [384], P('dp')
- w_up: bfloat16 [384, 1536], P('dp')
- b_up: bfloat16 [1536], P('dp')
- w_down: bfloat16 [1536, 384], P('dp')
- b_down: bfloat16 [384], P('dp')
Outputs:
- output: bfloat16 [512, 256, 384], P(('rep', 'dp')), parts along dimension 0
There are 2 independent parts. The reference program is written for one: setup_inputs(seed, part) draws one part's arguments, and reference() takes and returns one part's arrays. A program takes and returns all parts, laid end to end along the dimension named above; an argument that names none is the same for every part.
All inputs are finite; a program needn't handle non-finite values.
Results may differ from the reference program's by a relative error of at most 0.00971256.
Values are sent between devices in bfloat16 or wider.
A program may use at most 768 MiB of HBM per device.

```python
import jax
import jax.numpy as jnp
from jax import lax

N_IMAGES = 256
TOKENS = 256
PATCH_DIM = 588
WIDTH = 384
NUM_HEADS = 6
HEAD_DIM = 64
MLP_WIDTH = 1536
NORM_EPS = 1e-6


def draw_normal(sub_key, shape, scale, offset=0.0):
    values = offset + scale * jax.random.normal(sub_key, shape, jnp.float32)
    return values.astype(jnp.bfloat16)


def setup_inputs(seed: int = 0, part: int = 0) -> dict:
    root_key = jax.random.key(seed)
    image_key = jax.random.fold_in(jax.random.key(seed + 1), part)
    sub_keys = jax.random.split(root_key, 15)
    return {
        "patches": draw_normal(image_key, (N_IMAGES, TOKENS, PATCH_DIM), 1.0),
        "w_patch": draw_normal(sub_keys[0], (PATCH_DIM, WIDTH), PATCH_DIM ** -0.5),
        "b_patch": draw_normal(sub_keys[1], (WIDTH,), 0.5),
        "pos_emb": draw_normal(sub_keys[2], (TOKENS, WIDTH), 0.5),
        "ln_scale": draw_normal(sub_keys[3], (WIDTH,), 0.2, 1.0),
        "w_q": draw_normal(sub_keys[4], (WIDTH, WIDTH), WIDTH ** -0.5),
        "w_k": draw_normal(sub_keys[5], (WIDTH, WIDTH), WIDTH ** -0.5),
        "w_v": draw_normal(sub_keys[6], (WIDTH, WIDTH), WIDTH ** -0.5),
        "q_scale": draw_normal(sub_keys[7], (HEAD_DIM,), 0.3, 1.3),
        "k_scale": draw_normal(sub_keys[8], (HEAD_DIM,), 0.3, 1.3),
        "w_out": draw_normal(sub_keys[9], (WIDTH, WIDTH), WIDTH ** -0.5),
        "b_out": draw_normal(sub_keys[10], (WIDTH,), 0.3),
        "w_up": draw_normal(sub_keys[11], (WIDTH, MLP_WIDTH), WIDTH ** -0.5),
        "b_up": draw_normal(sub_keys[12], (MLP_WIDTH,), 0.5),
        "w_down": draw_normal(sub_keys[13], (MLP_WIDTH, WIDTH), MLP_WIDTH ** -0.5),
        "b_down": draw_normal(sub_keys[14], (WIDTH,), 0.3),
    }


def layer_norm(x_f32, scale):
    mean = jnp.mean(x_f32, axis=-1, keepdims=True)
    centered = x_f32 - mean
    variance = jnp.mean(centered * centered, axis=-1, keepdims=True)
    return centered * lax.rsqrt(variance + NORM_EPS) * scale.astype(jnp.float32)


def reference(patches, w_patch, b_patch, pos_emb, ln_scale, w_q, w_k, w_v, q_scale, k_scale, w_out, b_out, w_up, b_up, w_down, b_down):
    def one_image(image):
        embed = (jnp.dot(image, w_patch, preferred_element_type=jnp.float32) + b_patch.astype(jnp.float32) + pos_emb.astype(jnp.float32)).astype(jnp.bfloat16)
        embed_f32 = embed.astype(jnp.float32)
        normed = layer_norm(embed_f32, ln_scale).astype(jnp.bfloat16)

        def project(weight):
            projected = jnp.dot(normed, weight, preferred_element_type=jnp.float32).astype(jnp.bfloat16)
            return projected.reshape(TOKENS, NUM_HEADS, HEAD_DIM)

        queries = layer_norm(project(w_q).astype(jnp.float32), q_scale).astype(jnp.bfloat16)
        key_heads = layer_norm(project(w_k).astype(jnp.float32), k_scale).astype(jnp.bfloat16)
        values = project(w_v)
        scores = jnp.einsum("qhd,khd->hqk", queries.astype(jnp.float32), key_heads.astype(jnp.float32)) * HEAD_DIM ** -0.5
        attn_probs = jax.nn.softmax(scores, axis=-1).astype(jnp.bfloat16)
        attended = jnp.einsum("hqk,khd->qhd", attn_probs.astype(jnp.float32), values.astype(jnp.float32)).astype(jnp.bfloat16).reshape(TOKENS, WIDTH)
        attn_out = jnp.dot(attended, w_out, preferred_element_type=jnp.float32) + b_out.astype(jnp.float32)
        hidden = jnp.dot(normed, w_up, preferred_element_type=jnp.float32) + b_up.astype(jnp.float32)
        hidden = jax.nn.gelu(hidden, approximate=False).astype(jnp.bfloat16)
        mlp_out = jnp.dot(hidden, w_down, preferred_element_type=jnp.float32) + b_down.astype(jnp.float32)
        return (embed_f32 + attn_out + mlp_out).astype(jnp.bfloat16)

    return lax.map(one_image, patches)
```

```python
import functools
import math

import jax
import jax.numpy as jnp
from jax import lax
from jax.experimental import pallas as pl
from jax.experimental.pallas import tpu as pltpu
from jax.sharding import PartitionSpec as P

NORM_EPS = 1e-6
MESH = pl.DeviceIdType.MESH
BF16, F32 = jnp.bfloat16, jnp.float32
LANES = 128
GROUP = 8
ATTEND = 4
AHEAD = 2
MLP = 2
ONES_ROWS = 16
CORES = 2
VMEM_LIMIT = 60 * 1024 * 1024


def columns(row):
    return jnp.broadcast_to(row, (LANES, row.shape[1])).T


def norm_rows(x, gain):
    count = x.shape[0]
    mean = jnp.sum(x, axis=0, keepdims=True) * (1.0 / count)
    centered = x - mean
    variance = jnp.sum(centered * centered, axis=0, keepdims=True) * (1.0 / count)
    return centered * lax.rsqrt(variance + NORM_EPS) * gain


class Gather:
    def __init__(self, index, src, place, send, recv):
        self.index, self.src, self.place, self.send, self.recv = index, src, place, send, recv

    def copy(self, hop, src, block, target):
        return pltpu.make_async_remote_copy(
            src_ref=src, dst_ref=self.place(block), send_sem=self.send.at[self.index, hop],
            recv_sem=self.recv.at[self.index, hop], device_id={"dp": target}, device_id_type=MESH)


class Ring:
    def __init__(self, n):
        me = lax.axis_index("dp")
        self.chips = n // CORES
        self.chip, self.core = me // CORES, lax.rem(me, CORES)
        self.me = me
        self.sibling = self.device(self.chip, 1 - self.core)
        self.right = self.device(self.chip + 1, self.core)
        self.left = self.device(self.chip + self.chips - 1, self.core)
        self.onward = self.device(self.chip + 1 + self.core * (self.chips - 2), self.core)
        self.passed = self.device(self.chip + self.chips - 1 + self.core * (2 - self.chips), self.core)
        self.across = self.device(self.chip + 2, self.core)

    def device(self, chip, core):
        return lax.rem(chip, self.chips) * CORES + core

    def twin(self, device):
        return device + 1 - 2 * lax.rem(device, CORES)

    def start_own(self, items):
        for item in items:
            item.copy(1, item.src, self.me, self.right).start()
            item.copy(2, item.src, self.me, self.left).start()
            item.copy(0, item.src, self.me, self.sibling).start()

    def relay_near(self, items):
        for item in items:
            item.copy(1, item.src, self.left, self.right).wait_recv()
            item.copy(2, item.src, self.right, self.left).wait_recv()
            item.copy(5, item.place(self.passed), self.passed, self.onward).start()
            item.copy(3, item.place(self.left), self.left, self.sibling).start()
            item.copy(4, item.place(self.right), self.right, self.sibling).start()

    def relay_far(self, items):
        for item in items:
            item.copy(5, item.src, self.across, self.onward).wait_recv()
            item.copy(6, item.place(self.across), self.across, self.sibling).start()

    def finish(self, items):
        for item in items:
            for hop, block in ((0, self.me), (3, self.left), (4, self.right), (6, self.across)):
                item.copy(hop, item.src, self.twin(block), self.sibling).wait_recv()

    def drain(self, items):
        for item in items:
            for hop in range(7):
                item.copy(hop, item.src, self.me, self.sibling).wait_send()

    def barrier(self):
        semaphore = pltpu.get_barrier_semaphore()
        for other in (self.sibling, self.right, self.left):
            pl.semaphore_signal(semaphore, inc=1, device_id={"dp": other}, device_id_type=MESH)
        pl.semaphore_wait(semaphore, 3)


def first_kernel(n, heads, patches, wp, misc, wq, wk, wv, wo, wup, wdown, qs, ks,
                 e_out, h_out, o_out, w1_out, w2_out, vec_out,
                 g_wp, g_misc, g_q, g_k, g_v, g_o, g_u, g_d, w_qkv, bias_pos, gains, head_gains,
                 h_all, raw, q_pad, k_rows, v_ext, s_buf, p_buf, send, recv):
    step = pl.program_id(0)
    images, width, tokens = h_all.shape
    depth, group, _ = patches.shape
    slots = o_out.shape[0]
    embed_steps, attend_steps = images // group, images // slots
    head_dim = width // heads
    ring = Ring(n)

    def rows_of(ref, count):
        return lambda block: ref.at[pl.ds(pl.multiple_of(block * count, count), count), :]

    sources = (wp, misc, wq, wk, wv, wo, wup, wdown)
    targets = (g_wp, g_misc, g_q, g_k, g_v, g_o, g_u, g_d)
    items = [Gather(i, s, rows_of(t, s.shape[0]), send, recv) for i, (s, t) in enumerate(zip(sources, targets))]
    embed_items, qkv_items, late_items = items[:2], items[2:5], items[5:]

    def keep_own(some):
        for item in some:
            item.place(ring.me)[...] = item.src[...]

    @pl.when(step == 0)
    def _():
        ring.barrier()
        ring.start_own(embed_items)
        keep_own(items)
        ring.relay_near(embed_items)
        ring.start_own(qkv_items)
        ring.relay_far(embed_items)
        ring.finish(embed_items)
        pos_rows = tokens // n
        pos = jnp.concatenate([g_misc[b * misc.shape[0]:b * misc.shape[0] + pos_rows, :] for b in range(n)], axis=0).astype(F32)
        small = jnp.concatenate([g_misc[b * misc.shape[0] + pos_rows:(b + 1) * misc.shape[0], :].astype(F32)[0:1] for b in range(n)], axis=0)
        small = jnp.concatenate([small, jnp.zeros((LANES - n, width), F32)], axis=0).T
        piece = width // n

        def spread(first, count, b):
            return jnp.broadcast_to(small[first:first + count, b:b + 1], (count, LANES))

        for b in range(n):
            here = slice(b * piece, (b + 1) * piece)
            gains[0, here, :] = spread(0, piece, b)
            gains[1, here, :] = spread(piece, piece, b)
            vec_out[here, :] = spread(2 * piece, piece, b) + spread(3 * piece, piece, b)
            start = width + b * 4 * piece
            vec_out[start:start + 4 * piece, :] = spread(4 * piece, 4 * piece, b)
        pos_t = pos.T
        for i in range(tokens // LANES):
            bias_pos[:, i * LANES:(i + 1) * LANES] = gains[0] + pos_t[:, i * LANES:(i + 1) * LANES]
        head_gains[0] = columns(qs[...].astype(F32))[:head_dim]
        head_gains[1] = columns(ks[...].astype(F32))[:head_dim]
        v_ext[...] = jnp.ones_like(v_ext)
        q_pad[...] = jnp.zeros_like(q_pad)

    @pl.when(step == 1)
    def _():
        ring.relay_near(qkv_items)
        ring.start_own(late_items)

    @pl.when(step == embed_steps - 1)
    def _():
        ring.relay_far(qkv_items)

    @pl.when(step < embed_steps)
    def _():
        by_image = jnp.swapaxes(patches[...], 0, 1)
        for image in range(group):
            acc = jnp.dot(g_wp[:, :depth], by_image[image], preferred_element_type=F32)
            for lane in range(0, tokens, LANES):
                at = slice(lane, lane + LANES)
                e = (acc[:, at] + bias_pos[:, at]).astype(BF16)
                e_out[image, :, at] = e
                h = norm_rows(e.astype(F32), gains[1]).astype(BF16)
                h_all[step * group + image, :, at] = h
                h_out[image, :, at] = h

    scale = head_dim ** -0.5 * math.log2(math.e)
    units = slots * heads

    def project(kind, image, slot):
        out = jnp.dot(w_qkv[kind], h_all[image], preferred_element_type=F32).astype(BF16)
        if kind < 2:
            raw[slot, kind] = out
        else:
            for head in range(heads):
                v_ext[slot, head, :head_dim, :] = out[head * head_dim:(head + 1) * head_dim, :]

    def norm_heads(slot, couple):
        for lane in range(0, tokens, LANES):
            at = slice(lane, lane + LANES)
            keys = []
            for head in (2 * couple, 2 * couple + 1):
                rows = slice(head * head_dim, (head + 1) * head_dim)
                place = (head % 2) * head_dim
                q_pad[slot, head, place:place + head_dim, at] = norm_rows(raw[slot, 0, rows, at].astype(F32), head_gains[0]).astype(BF16)
                keys.append(norm_rows(raw[slot, 1, rows, at].astype(F32), head_gains[1]).astype(BF16))
            k_rows[slot, couple, at, :] = jnp.concatenate(keys, axis=0).T

    def score(unit):
        slot, head = divmod(unit % units, heads)
        s_buf[unit % s_buf.shape[0]] = jnp.dot(k_rows[slot, head // 2], q_pad[slot, head], preferred_element_type=F32)

    def soften(unit):
        for lane in range(0, tokens, LANES):
            at = slice(lane, lane + LANES)
            s = s_buf[unit % s_buf.shape[0], :, at]
            top = jnp.max(s, axis=0, keepdims=True)
            p_buf[unit % p_buf.shape[0], :, at] = jnp.exp2((s - top) * scale).astype(BF16)

    def attend(unit):
        slot, head = divmod(unit, heads)
        o = jnp.dot(v_ext[slot, head], p_buf[unit % p_buf.shape[0]], preferred_element_type=F32)
        o_out[slot, head * head_dim:(head + 1) * head_dim, :] = (o[:head_dim] * (1.0 / o[head_dim:head_dim + 1])).astype(BF16)

    @pl.when(step == embed_steps)
    def _():
        ring.finish(qkv_items)
        for i, ref in enumerate((g_q, g_k, g_v)):
            w_qkv[i] = ref[...].T
        ring.relay_near(late_items)
        for kind in range(3):
            project(kind, 0, 0)
        for couple in range(heads // 2):
            norm_heads(0, couple)
        for unit in range(AHEAD):
            score(unit)
        soften(0)

    @pl.when(step == embed_steps + attend_steps // 2)
    def _():
        ring.relay_far(late_items)

    @pl.when(step == embed_steps + attend_steps - 2)
    def _():
        ring.finish(late_items)
        ring.drain(items)
        w1_out[...] = g_u[...].T
        w2_out[:, :width] = g_o[...].T
        w2_out[:, width:] = g_d[...].T

    @pl.when(step >= embed_steps)
    def _():
        first = (step - embed_steps) * slots
        for slot in range(slots):
            following = jnp.minimum(first + slot + 1, images - 1)
            target = (slot + 1) % slots
            for head in range(heads):
                unit = slot * heads + head
                if head == 0:
                    project(0, following, target)
                    project(1, following, target)
                if head == 1:
                    project(2, following, target)
                score(unit + AHEAD)
                soften(unit + 1)
                if 1 <= head <= heads // 2:
                    norm_heads(target, head - 1)
                attend(unit)


def second_kernel(e, h, o, w1, w2, vec, y, z):
    images, tokens, width = y.shape
    hidden = w1.shape[0]
    root_half = math.sqrt(0.5)
    for image in range(images):
        z[image, :width, :] = o[image]
        for first in range(0, hidden, width):
            u = jnp.dot(w1[first:first + width, :], h[image], preferred_element_type=F32)
            for lane in range(0, tokens, LANES):
                x = u[:, lane:lane + LANES] + vec[width + first:2 * width + first, :]
                half = 0.5 * x
                z[image, width + first:2 * width + first, lane:lane + LANES] = (half + half * lax.erf(x * root_half)).astype(BF16)
    for image in range(images):
        acc = jnp.dot(w2[...], z[image], preferred_element_type=F32)
        for lane in range(0, tokens, LANES):
            at = slice(lane, lane + LANES)
            out = acc[:, at] + vec[:width, :] + e[image, :, at].astype(F32)
            y[image, at, :] = out.astype(BF16).T


def solution(mesh):
    n = mesh.shape["dp"]
    act_spec = P(("rep", "dp"), None, None)
    row_spec = P("dp", None)
    vec_spec = P("dp")
    in_specs = (act_spec, P(None, "dp"), vec_spec, row_spec, vec_spec, row_spec, row_spec, row_spec, P(None), P(None), row_spec, vec_spec, row_spec, vec_spec, row_spec, vec_spec)

    def per_device(patches, w_patch, b_patch, pos_emb, ln_scale, w_q, w_k, w_v, q_scale, k_scale, w_out, b_out, w_up, b_up, w_down, b_down):
        images, tokens, depth = patches.shape
        width = w_q.shape[1]
        hidden = w_up.shape[1]
        head_dim = q_scale.shape[0]
        heads = width // head_dim
        padded = -(-depth // LANES) * LANES
        wp = jnp.pad(w_patch.T, ((0, 0), (0, padded - depth)))
        small = jnp.concatenate([b_patch, ln_scale, b_out, b_down, b_up])
        small = jnp.pad(small[None, :], ((0, 15), (0, width - small.shape[0])))
        misc = jnp.concatenate([pos_emb, small], axis=0)

        whole = pl.BlockSpec(memory_space=pltpu.VMEM)
        embed_steps = images // GROUP
        attend_steps = images // ATTEND
        early = lambda s: (jnp.minimum(s, embed_steps - 1), 0, 0)
        late = lambda s: (jnp.maximum(s - embed_steps, 0), 0, 0)
        act = jax.ShapeDtypeStruct((images, width, tokens), BF16)
        shards = (wp, misc, w_q, w_k, w_v, w_out, w_up, w_down)
        e, h, o, w1, w2, vec = pl.pallas_call(
            functools.partial(first_kernel, n, heads),
            grid=(embed_steps + attend_steps,),
            out_shape=(act, act, act,
                       jax.ShapeDtypeStruct((hidden, width), BF16),
                       jax.ShapeDtypeStruct((width, width + hidden), BF16),
                       jax.ShapeDtypeStruct((width + hidden, LANES), F32)),
            in_specs=[pl.BlockSpec((depth, GROUP, tokens), lambda s: (0, jnp.minimum(s, embed_steps - 1), 0))] + [whole] * 10,
            out_specs=[pl.BlockSpec((GROUP, width, tokens), early)] * 2 + [
                       pl.BlockSpec((ATTEND, width, tokens), late), whole, whole, whole],
            scratch_shapes=[pltpu.VMEM((n * s.shape[0], s.shape[1]), BF16) for s in shards] + [
                pltpu.VMEM((3, width, width), BF16),
                pltpu.VMEM((width, tokens), F32),
                pltpu.VMEM((2, width, LANES), F32),
                pltpu.VMEM((2, head_dim, LANES), F32),
                pltpu.VMEM((images, width, tokens), BF16),
                pltpu.VMEM((ATTEND, 2, width, tokens), BF16),
                pltpu.VMEM((ATTEND, heads, 2 * head_dim, tokens), BF16),
                pltpu.VMEM((ATTEND, heads // 2, tokens, 2 * head_dim), BF16),
                pltpu.VMEM((ATTEND, heads, head_dim + ONES_ROWS, tokens), BF16),
                pltpu.VMEM((3, tokens, tokens), F32),
                pltpu.VMEM((2, tokens, tokens), BF16),
                pltpu.SemaphoreType.DMA((len(shards), 7)),
                pltpu.SemaphoreType.DMA((len(shards), 7)),
            ],
            compiler_params=pltpu.CompilerParams(collective_id=0, has_side_effects=True, vmem_limit_bytes=VMEM_LIMIT),
        )(jnp.transpose(patches, (2, 0, 1)), *shards, q_scale[None, :], k_scale[None, :])
        block = pl.BlockSpec((MLP, width, tokens), lambda s: (s, 0, 0))
        return pl.pallas_call(
            second_kernel,
            grid=(images // MLP,),
            out_shape=jax.ShapeDtypeStruct((images, tokens, width), BF16),
            in_specs=[block] * 3 + [whole] * 3,
            out_specs=pl.BlockSpec((MLP, tokens, width), lambda s: (s, 0, 0)),
            scratch_shapes=[pltpu.VMEM((MLP, width + hidden, tokens), BF16)],
            compiler_params=pltpu.CompilerParams(vmem_limit_bytes=VMEM_LIMIT),
        )(e, h, o, w1, w2, vec)

    return jax.shard_map(per_device, mesh=mesh, in_specs=in_specs, out_specs=act_spec, check_vma=False)
```
